128 devices in a mesh: gx: 4 (over x), gy: 32 (over z, y, core).
Axes of the slice: x: 4, y: 4, z: 4, core: 2. Of those that a mesh axis runs over, the one named last changes fastest.
Arguments:
- schur_blocks: float32 [128, 2048, 2048], P(('gx', 'gy')), may hold values from -1 to 11, as said below
- offsets: int32 [128], P(('gx', 'gy')), may hold values from 256 to 768, as said below
- right_side: float32 [131072, 128], P(('gx', 'gy')), may hold values from -20 to 20
- coarse_basis: float32 [131072, 128], P(('gx', 'gy')), may hold values from -0.015625 to 0.015625
- coarse_load: float32 [128, 128], replicated, may hold values from -6 to 6
Outputs:
- multipliers: float32 [131072, 128], P(('gx', 'gy'))
- amplitudes: float32 [128, 128], replicated
The draws below stay inside these ranges and needn't reach their ends.
Inputs may be any that keep to these rules, and one draw needn't show every extreme that they name: `schur_blocks`: each block is symmetric positive definite. `offsets`: both ends of the range are taken by some subdomain.
All inputs are finite; a program needn't handle non-finite values.
Results may differ from the reference program's by a relative error of at most 0.0003.
Values sent between devices are 32-bit elements; how exact they have to be, the bound alone decides.
A program may use at most 128 MiB of HBM per device.

```python
import math
import jax
import jax.numpy as jnp
from jax import lax

W = 2048
SLAB = 1024
R = 128
NC = 128
ITERS = 3
SUBDOMAINS = 128
MULTS = 131072


def draw_schur_blocks(key, part):
    upper_end = 4.0
    subkeys = jax.random.split(key, SUBDOMAINS)

    def single(subkey):
        diag_key, noise_key = jax.random.split(subkey)
        diagonal = jnp.exp(jax.random.uniform(diag_key, (W,), jnp.float32, 0.0, math.log(upper_end)))
        noise_part = jax.random.truncated_normal(noise_key, -5.0, 5.0, (W, W), jnp.float32) * (0.25 / math.sqrt(W))
        return jnp.diag(diagonal) + (noise_part + noise_part.T) * 0.7071067811865476
    return lax.map(single, subkeys)


def draw_offsets(key, part):
    key_values, key_ranking = jax.random.split(key)
    lowest = SLAB // 4
    highest = 3 * SLAB // 4
    values = jax.random.randint(key_values, (SUBDOMAINS,), lowest, highest + 1).astype(jnp.int32)
    ranking = jax.random.permutation(key_ranking, SUBDOMAINS)
    values = values.at[ranking[0]].set(lowest).at[ranking[1]].set(highest)
    return values.astype(jnp.int32)


def draw_right_side(key, part):
    base_key = jax.random.fold_in(key, 0)
    total_rows = SLAB * SUBDOMAINS
    position = jnp.arange(total_rows, dtype=jnp.float32) / total_rows
    base = jax.random.truncated_normal(base_key, -4.0, 4.0, (total_rows, R), jnp.float32)
    rising = 1.0 + 2.0 * position
    return base * rising[:, None]


def block_scale(stream_key, dims, cuts, low, top_value):
    gain, own = 1.0, jax.random.fold_in(stream_key, 6)
    for dim, shards_of in cuts:
        heights = jnp.exp(jax.random.uniform(jax.random.fold_in(own, dim), (shards_of,), jnp.float32, low / len(cuts), top_value / len(cuts)))
        gain = gain * jnp.repeat(heights, dims[dim] // shards_of).reshape([-1 if axis == dim else 1 for axis in range(len(dims))])
    return gain


def gaussian(stream_key, extent, spread, reach, pieces=(), kind=jnp.bfloat16):
    values = jax.random.normal(stream_key, extent, jnp.float32) * spread
    if len(pieces) > 0:
        values = block_scale(stream_key, extent, pieces, -0.22, 0.18) * values
    return jnp.clip(values, min=-reach, max=reach).astype(kind)


def setup_inputs(seed: int = 0) -> dict:
    keys = jax.random.split(jax.random.key(seed), 6)
    return {
        "schur_blocks": draw_schur_blocks(jax.random.fold_in(keys[5], 71), 0),
        "offsets": draw_offsets(jax.random.fold_in(keys[5], 71), 0),
        "right_side": draw_right_side(jax.random.fold_in(keys[5], 71), 0),
        "coarse_basis": gaussian(keys[3], (MULTS, NC), MULTS ** -0.5, 0.015625, ((0, 128),), jnp.float32),
        "coarse_load": gaussian(keys[4], (NC, R), 1.0, 6.0, (), jnp.float32),
    }


HIGHEST = lax.Precision.HIGHEST

def apply_operator(vector, schur_blocks, offsets):
    padded = jnp.pad(vector, ((SLAB, SLAB), (0, 0)))

    def visit_block(accumulated, inputs):
        schur_block, start_row, device_index = inputs
        first_row = (device_index * SLAB + start_row).astype(jnp.int32)
        window = lax.dynamic_slice_in_dim(padded, first_row, W, 0)
        product_block = jnp.dot(schur_block.astype(jnp.float32), window.astype(jnp.float32), precision=HIGHEST, preferred_element_type=jnp.float32)
        current = lax.dynamic_slice_in_dim(accumulated, first_row, W, 0)
        return (lax.dynamic_update_slice_in_dim(accumulated, current + product_block, first_row, 0), None)
    indices = jnp.arange(SUBDOMAINS, dtype=jnp.int32)
    accumulated, _ = lax.scan(visit_block, jnp.zeros_like(padded), (schur_blocks, offsets.astype(jnp.int32), indices))
    return accumulated[SLAB:SLAB + vector.shape[0]]

def project(residual, coarse_basis, gram_factor):
    coarse_part = jnp.dot(coarse_basis.T.astype(jnp.float32), residual.astype(jnp.float32), precision=HIGHEST, preferred_element_type=jnp.float32)
    amplitudes = jax.scipy.linalg.cho_solve((gram_factor, True), coarse_part)
    projected = residual - jnp.dot(coarse_basis.astype(jnp.float32), amplitudes.astype(jnp.float32), precision=HIGHEST, preferred_element_type=jnp.float32)
    return (projected, amplitudes)

def reference(schur_blocks, offsets, right_side, coarse_basis, coarse_load):
    gram_matrix = jnp.dot(coarse_basis.T.astype(jnp.float32), coarse_basis.astype(jnp.float32), precision=HIGHEST, preferred_element_type=jnp.float32)
    gram_factor = jnp.linalg.cholesky(gram_matrix)
    start_load = jax.scipy.linalg.cho_solve((gram_factor, True), coarse_load)
    multipliers = jnp.dot(coarse_basis.astype(jnp.float32), start_load.astype(jnp.float32), precision=HIGHEST, preferred_element_type=jnp.float32)
    residual = right_side - apply_operator(multipliers, schur_blocks, offsets)
    projected, amplitudes = project(residual, coarse_basis, gram_factor)
    direction = projected
    energy_now = jnp.sum(projected * projected, axis=0)
    for iteration in range(ITERS):
        operator_image = apply_operator(direction, schur_blocks, offsets)
        step_length = energy_now / jnp.sum(direction * operator_image, axis=0)
        multipliers = multipliers + step_length * direction
        residual = residual - step_length * operator_image
        projected, amplitudes = project(residual, coarse_basis, gram_factor)
        energy_next = jnp.sum(projected * projected, axis=0)
        direction = projected + energy_next / energy_now * direction
        energy_now = energy_next
    return (multipliers, amplitudes)
```

```python
import functools

import jax
import jax.numpy as jnp
from jax import lax
from jax.experimental import pallas as pl
from jax.experimental.pallas import tpu as pltpu
from jax.sharding import Mesh
from jax.sharding import PartitionSpec as P


ITERS = 3
R = 128
AXES = ("gx", "gy_0", "gy_1", "gy_2")
MESH = pl.DeviceIdType.MESH
F32, BF16 = jnp.float32, jnp.bfloat16
HIGHEST = lax.Precision.HIGHEST
SLOTS = 4
N_AR = 2 + ITERS


def halves(x):
    high = x.astype(BF16)
    low = (x - high.astype(F32)).astype(BF16)
    return high, low


def wide(x):
    return jnp.concatenate(halves(x), axis=1)


def stacked(x):
    both = wide(x)
    return jnp.concatenate([both, both], axis=0)


def fold(acc):
    return acc[:, :R] + acc[:, R:]


def dot(a, b):
    return jnp.dot(a, b, preferred_element_type=F32)


def exact(a, b):
    return jnp.dot(a, b, precision=HIGHEST, preferred_element_type=F32)


def kernel(
    dims,
    slab,
    s_hbm,
    off_ref,
    rhs_hbm,
    b_hbm,
    load_ref,
    mult_ref,
    amp_ref,
    s_in,
    ss,
    b_own,
    r_own,
    hb,
    hr,
    ta,
    ha,
    wo,
    hw,
    e3,
    vv,
    y4,
    yy,
    rr,
    st,
    dd,
    bx,
    bto,
    btw,
    gm,
    mat1,
    cb1,
    own1,
    slot1,
    full1,
    mat2,
    cb2,
    own2,
    slot2,
    full2,
    in_sem,
    s_sem,
    ar_send,
    ar_recv,
    halo_send,
    halo_recv,
    a_send,
    a_recv,
    b_send,
    b_recv,
):
    nx, nz, ny, nc = dims
    count = nx * nz * ny * nc
    window = 2 * slab
    q = slab // 4
    half = R // 2 + 8
    x, z, y, c = (lax.axis_index(a) for a in AXES)
    me = ((x * nz + z) * ny + y) * nc + c
    first, last = me == 0, me == count - 1

    def place(line):
        return (
            line // (nz * ny * nc),
            (line // (ny * nc)) % nz,
            (line // nc) % ny,
            line % nc,
        )

    right = place((me + 1) % count)
    left = place((me + count - 1) % count)
    partner = (x, z, y, (c + 1) % nc)
    rings = {
        "y": [(x, z, (y + k) % ny, c) for k in range(1, ny)],
        "x": [((x + k) % nx, z, y, c) for k in range(1, nx)],
        "z": [(x, (z + k) % nz, y, c) for k in range(1, nz)],
    }
    peers = [left, right, partner] + rings["y"] + rings["x"] + rings["z"]

    def remote(src, dst, send, recv, device):
        return pltpu.make_async_remote_copy(
            src_ref=src, dst_ref=dst, send_sem=send, recv_sem=recv, device_id=device, device_id_type=MESH
        )

    pending = []

    def launch(copies):
        for copy in copies:
            copy.start()
        pending.extend(copies)

    class Reduction:
        def __init__(self, index, mat, cb, own, slot, full, rows):
            self.base = index * 11
            self.mat, self.cb, self.own, self.slot, self.full, self.rows = mat, cb, own, slot, full, rows
            self.order = ("y", "x", "z")
            self.step = 0
            self.flying = None

        def sems(self, k):
            return ar_send.at[self.base + k], ar_recv.at[self.base + k]

        def start(self):
            n = self.rows
            copy = remote(self.mat.at[pl.ds((1 - c) * n, n)], self.cb, *self.sems(0), partner)
            launch([copy])
            self.flying = [copy]

        def arrived(self):
            for copy in self.flying:
                copy.wait_recv()
            if self.step == 0:
                return self.mat[pl.ds(c * self.rows, self.rows), :] + self.cb[...]
            j = self.step - 1
            mine = self.own[j]
            got = [self.slot[j, k] for k in range(len(self.flying))]
            if len(got) == 1:
                return mine + got[0]
            return (mine + got[1]) + (got[0] + got[2])

        def ring(self):
            total = self.arrived()
            j = self.step
            self.own[j] = total
            copies = []
            for k, device in enumerate(rings[self.order[j]]):
                copies.append(remote(self.own.at[j], self.slot.at[j, k], *self.sems(1 + j * 3 + k), device))
            launch(copies)
            self.flying = copies
            self.step += 1

        def last(self):
            n = self.rows
            total = self.arrived()
            self.full[pl.ds(c * n, n), :] = total
            piece = self.full.at[pl.ds(c * n, n)]
            copy = remote(piece, piece, *self.sems(10), partner)
            launch([copy])
            self.flying = [copy]

        def result(self):
            self.flying[0].wait_recv()
            return self.full

    first_sum = Reduction(0, mat1, cb1, own1, slot1, full1, R)
    sums = [
        Reduction(1 + i, mat2.at[i], cb2.at[i], own2.at[i], slot2.at[i], full2.at[i], half)
        for i in range(1 + ITERS)
    ]

    def whole_halo(own, into, k):
        return [
            remote(own.at[pl.ds(q, 3 * q)], into.at[0, pl.ds(q, 3 * q)], halo_send.at[k], halo_recv.at[k], right),
            remote(own.at[pl.ds(0, 3 * q)], into.at[1, pl.ds(0, 3 * q)], halo_send.at[k + 1], halo_recv.at[k + 1], left),
        ]

    def to_right(i, k):
        rows, sem = pl.ds(k * q, q), 6 * i + k
        return remote(ta.at[i, 0, rows], ha.at[i, 0, rows], a_send.at[sem], a_recv.at[sem], right)

    def to_left(i, k):
        rows, sem = pl.ds(k * q, q), 6 * i + 2 + k
        return remote(ta.at[i, 1, rows], ha.at[i, 1, rows], a_send.at[sem], a_recv.at[sem], left)

    def image_right(i, k):
        rows, sem = pl.ds(k * q, q), 6 * i + k - 1
        return remote(wo.at[i, rows], hw.at[i, 0, rows], b_send.at[sem], b_recv.at[sem], right)

    def image_left(i, k):
        rows, sem = pl.ds(k * q, q), 6 * i + 3 + k
        return remote(wo.at[i, rows], hw.at[i, 1, rows], b_send.at[sem], b_recv.at[sem], left)

    b_in = pltpu.make_async_copy(b_hbm, b_own, in_sem.at[0])
    r_in = pltpu.make_async_copy(rhs_hbm, r_own, in_sem.at[1])
    b_in.start()
    r_in.start()
    strip = window // 8

    def strip_in(i):
        return pltpu.make_async_copy(s_hbm.at[0, pl.ds(i * strip, strip)], s_in.at[i % SLOTS], s_sem.at[i % SLOTS])

    for i in range(SLOTS):
        strip_in(i).start()
    barrier = pltpu.get_barrier_semaphore()
    for device in peers:
        pl.semaphore_signal(barrier, inc=1, device_id=device, device_id_type=MESH)

    off = off_ref[0]
    row_of = lax.broadcasted_iota(jnp.int32, (q, R), 0)

    def from_sides(lower, upper, k):
        lower = None if lower is None else jnp.where(first, 0.0, lower)
        upper = None if upper is None else jnp.where(last, 0.0, upper)
        if k == 0:
            return upper
        if k == 3:
            return lower
        return jnp.where(row_of + k * q < off, upper, lower)

    def halo_rows(ref, k):
        rows = pl.ds(k * q, q)
        lower = ref[0, rows, :] if k > 0 else None
        upper = ref[1, rows, :] if k < 3 else None
        return from_sides(lower, upper, k)

    def put_own(k, value):
        e3[slab + k * q : slab + (k + 1) * q, :] = value

    def put_halo(k, value):
        e3[k * q : (k + 1) * q, :] = value
        e3[2 * slab + k * q : 2 * slab + (k + 1) * q, :] = value

    b_in.wait()
    for k in range(4):
        rows = slice(k * q, (k + 1) * q)
        value = b_own[rows, :]
        high, low = halves(value)
        bx[rows, :R] = high
        bx[rows, R:] = low
        across = value.T
        high, low = halves(across)
        bto[:R, rows] = high
        bto[R:, rows] = low
        put_own(k, value)
    r_in.wait()
    pl.semaphore_wait(barrier, len(peers))
    b_halo = whole_halo(b_own, hb, 0)
    launch(b_halo)

    def quarters(acc):
        return (acc[:R, :R] + acc[R:, R:]) + (acc[:R, R:] + acc[R:, :R])

    mat1[:R, :] = quarters(dot(bto[...], bx[:slab, :]))
    mat1[R:, :] = quarters(dot(bto[...], wide(r_own[...])))
    first_sum.start()

    def split_strip(i):
        strip_in(i).wait()
        rows = pl.ds(i * strip, strip)
        high, low = halves(s_in[i % SLOTS])
        ss[rows, :window] = high
        ss[rows, window:] = low
        if i + SLOTS < 8:
            strip_in(i + SLOTS).start()

    for i in range(3):
        split_strip(i)
    first_sum.ring()
    r_halo = whole_halo(r_own, hr, 2)
    launch(r_halo)
    for i in range(3, 6):
        split_strip(i)
    first_sum.ring()
    for i in range(6, 8):
        split_strip(i)
    first_sum.ring()

    for copy in b_halo:
        copy.wait_recv()
    for k in range(4):
        value = halo_rows(hb, k)
        rows = slice(slab + k * q, slab + (k + 1) * q)
        high, low = halves(value)
        bx[rows, :R] = high
        bx[rows, R:] = low
        put_halo(k, value)

    block = window // 4

    def split_vector(basis):
        for i in range(8):
            rows = slice(i * strip, (i + 1) * strip)
            value = e3[pl.ds(off + i * strip, strip), :]
            high, low = halves(value)
            vv[rows, :R] = high
            vv[rows, R:] = low
            again = slice(window + i * strip, window + (i + 1) * strip)
            vv[again, :R] = high
            vv[again, R:] = low
            if basis:
                high, low = halves(value.T)
                btw[:R, rows] = high
                btw[R:, rows] = low

    def apply_block(i, total):
        start = pl.multiple_of(i * block, block)
        rows = pl.ds(start, block)
        product = fold(dot(ss[rows, :], vv[...]))
        y4[rows, :] = product
        high, low = halves(product)
        yy[rows, :R] = high
        yy[rows, R:] = low
        value = e3[pl.ds(off + start, block), :]
        return total + jnp.sum((value * product).reshape(block // 8, 8, R), axis=0)

    def apply_operator():
        total = lax.fori_loop(0, window // block, apply_block, jnp.zeros((8, R), F32))
        y4[window : window + slab, :] = y4[:slab, :]
        return quarters(dot(btw[...], yy[...])), total

    def send_buffers(i):
        for k in range(4):
            value = y4[pl.ds(window - off + k * q, q), :]
            below = row_of + k * q < off
            rows = slice(k * q, (k + 1) * q)
            if k < 3:
                ta[i, 0, rows, :] = jnp.where(below, value, 0.0)
            if k > 0:
                ta[i, 1, rows, :] = jnp.where(below, 0.0, value)

    def send_contributions(i):
        launch([to_right(i, 1), to_left(i, 1), to_right(i, 2), to_left(i, 2), to_right(i, 0), to_left(i, 3)])

    def own_image(i, k):
        rows = slice(k * q, (k + 1) * q)
        value = y4[pl.ds(slab - off + k * q, q), :]
        if k < 3:
            to_right(i, k).wait_recv()
            value = value + jnp.where(first, 0.0, ha[i, 0, rows, :])
        if k > 0:
            to_left(i, k).wait_recv()
            value = value + jnp.where(last, 0.0, ha[i, 1, rows, :])
        wo[i, rows, :] = value
        copies = []
        if k > 0:
            copies.append(image_right(i, k))
        if k < 3:
            copies.append(image_left(i, k))
        launch(copies)

    def halo_image(i, k):
        if k > 0:
            image_right(i, k).wait_recv()
        if k < 3:
            image_left(i, k).wait_recv()
        return halo_rows(hw.at[i], k)

    line = lax.broadcasted_iota(jnp.int32, (R, R), 0)
    lane = lax.broadcasted_iota(jnp.int32, (R, R), 1)

    def eliminate(begin, end):
        a = gm[...]
        for k in range(begin, end):
            inverse = 1.0 / a[k : k + 1, k : k + 1]
            pivot = jnp.where(lane[:1] == k, 1.0, a[k : k + 1, :]) * inverse
            column = a[:, k : k + 1]
            a = jnp.where(line == k, pivot, jnp.where(lane == k, 0.0, a) - column * pivot)
        gm[...] = a

    split_vector(True)
    coarse_image, _ = apply_operator()
    total = sums[0]
    mat2[0, :R, :] = coarse_image
    mat2[0, R:, :] = jnp.zeros((2 * half - R, R), F32)
    total.start()
    send_buffers(0)
    first_sum.last()
    total.ring()
    send_contributions(0)
    gm[...] = first_sum.result()[:R, :]
    eliminate(0, 32)
    total.ring()
    own_image(0, 1)
    eliminate(32, 48)
    own_image(0, 2)
    eliminate(48, 64)
    own_image(0, 0)
    own_image(0, 3)
    total.ring()
    eliminate(64, 96)
    total.last()
    eliminate(96, 128)
    gram_inverse = gm[...]
    start_load = exact(gram_inverse, load_ref[...])
    basis_image = total.result()[:R, :]
    coarse = full1[R:, :] - exact(basis_image, start_load)
    amp = exact(gram_inverse, coarse)
    for copy in r_halo:
        copy.wait_recv()

    def rows_sum(value):
        return jnp.sum(value.reshape(q // 8, 8, R), axis=0)

    start_wide, amp_wide = stacked(start_load), stacked(amp)
    energy_part = jnp.zeros((8, R), F32)
    for k in range(8):
        rows = slice(k * q, (k + 1) * q)
        if k < 4:
            image, known = wo[0, rows, :], r_own[rows, :]
            mult_ref[rows, :] = fold(dot(bx[rows, :], start_wide))
        else:
            image, known = halo_image(0, k - 4), halo_rows(hr, k - 4)
        residual = known - fold(dot(wide(image), start_wide))
        rr[rows, :] = residual
        projected = residual - fold(dot(bx[rows, :], amp_wide))
        if k < 4:
            put_own(k, projected)
            dd[rows, :] = projected
            energy_part = energy_part + rows_sum(projected * projected)
        else:
            put_halo(k - 4, projected)

    sub = lax.broadcasted_iota(jnp.int32, (8, R), 0)
    mixed_part = jnp.zeros((8, R), F32)
    energy_old = curvature = basis_old = None
    for it in range(ITERS):
        more = it < ITERS - 1
        slot = 1 + it
        total = sums[slot]
        split_vector(False)
        basis_part, curve_part = apply_operator()
        scalars = [jnp.sum(v, axis=0, keepdims=True) for v in (energy_part, curve_part, mixed_part)]
        mat2[slot, :R, :] = basis_part
        mat2[slot, R : R + 8, :] = jnp.where(
            sub == 0, scalars[0], jnp.where(sub == 1, scalars[1], jnp.where(sub == 2, scalars[2], 0.0))
        )
        mat2[slot, R + 8 :, :] = jnp.zeros((2 * half - R - 8, R), F32)
        total.start()
        if more:
            send_buffers(slot)
        total.ring()
        if more:
            send_contributions(slot)
        total.ring()
        if more:
            own_image(slot, 1)
            own_image(slot, 2)
        total.ring()
        if more:
            own_image(slot, 0)
            own_image(slot, 3)
        total.last()
        got = total.result()
        basis_image = got[:R, :]
        energy = got[R : R + 1, :]
        curve = got[R + 1 : R + 2, :]
        mixed = got[R + 2 : R + 3, :]
        if it == 0:
            beta = None
            curvature = curve
        else:
            beta = energy / energy_old
            curvature = curve + beta * (2.0 * mixed + beta * curvature)
            basis_image = basis_image + beta * basis_old
        step = energy / curvature
        energy_old, basis_old = energy, basis_image
        coarse = coarse - step * basis_image
        amp = exact(gram_inverse, coarse)
        if not more:
            amp_ref[...] = amp
        amp_wide = stacked(amp)
        energy_part = jnp.zeros((8, R), F32)
        mixed_part = jnp.zeros((8, R), F32)
        for k in range(8 if more else 4):
            rows = slice(k * q, (k + 1) * q)
            if k < 4:
                direction = dd[rows, :]
                if it > 0:
                    direction = e3[slab + k * q : slab + (k + 1) * q, :] + beta * direction
                    dd[rows, :] = direction
                mult_ref[rows, :] = mult_ref[rows, :] + step * direction
                if not more:
                    continue
                image = wo[slot, rows, :]
            else:
                image = halo_image(slot, k - 4)
            if it > 0:
                image = image + beta * st[rows, :]
            st[rows, :] = image
            residual = rr[rows, :] - step * image
            rr[rows, :] = residual
            projected = residual - fold(dot(bx[rows, :], amp_wide))
            if k < 4:
                put_own(k, projected)
                energy_part = energy_part + rows_sum(projected * projected)
                mixed_part = mixed_part + rows_sum(projected * image)
            else:
                put_halo(k - 4, projected)
    for copy in pending:
        copy.wait_send()


def local(dims, schur_blocks, offsets, right_side, coarse_basis, coarse_load):
    slab = right_side.shape[0]
    window = 2 * slab
    half = R // 2 + 8
    vmem, dma = pltpu.VMEM, pltpu.SemaphoreType.DMA
    anywhere = pl.BlockSpec(memory_space=pl.ANY)
    local_vmem = pl.BlockSpec(memory_space=pltpu.VMEM)
    return pl.pallas_call(
        functools.partial(kernel, dims, slab),
        out_shape=(
            jax.ShapeDtypeStruct((slab, R), F32),
            jax.ShapeDtypeStruct((R, R), F32),
        ),
        in_specs=[anywhere, pl.BlockSpec(memory_space=pltpu.SMEM), anywhere, anywhere, local_vmem],
        out_specs=(local_vmem, local_vmem),
        scratch_shapes=[
            vmem((SLOTS, window // 8, window), F32),
            vmem((window, 2 * window), BF16),
            vmem((slab, R), F32),
            vmem((slab, R), F32),
            vmem((2, slab, R), F32),
            vmem((2, slab, R), F32),
            vmem((ITERS, 2, slab, R), F32),
            vmem((ITERS, 2, slab, R), F32),
            vmem((ITERS, slab, R), F32),
            vmem((ITERS, 2, slab, R), F32),
            vmem((3 * slab, R), F32),
            vmem((2 * window, 2 * R), BF16),
            vmem((window + slab, R), F32),
            vmem((window, 2 * R), BF16),
            vmem((window, R), F32),
            vmem((window, R), F32),
            vmem((slab, R), F32),
            vmem((window, 2 * R), BF16),
            vmem((2 * R, slab), BF16),
            vmem((2 * R, window), BF16),
            vmem((R, R), F32),
            vmem((2 * R, R), F32),
            vmem((R, R), F32),
            vmem((3, R, R), F32),
            vmem((3, 3, R, R), F32),
            vmem((2 * R, R), F32),
            vmem((1 + ITERS, 2 * half, R), F32),
            vmem((1 + ITERS, half, R), F32),
            vmem((1 + ITERS, 3, half, R), F32),
            vmem((1 + ITERS, 3, 3, half, R), F32),
            vmem((1 + ITERS, 2 * half, R), F32),
            dma((2,)),
            dma((SLOTS,)),
            dma((11 * N_AR,)),
            dma((11 * N_AR,)),
            dma((4,)),
            dma((4,)),
            dma((6 * ITERS,)),
            dma((6 * ITERS,)),
            dma((6 * ITERS,)),
            dma((6 * ITERS,)),
        ],
        compiler_params=pltpu.CompilerParams(
            collective_id=0, has_side_effects=True, vmem_limit_bytes=67000000
        ),
    )(schur_blocks, offsets, right_side, coarse_basis, coarse_load)


def solution(mesh):
    if "gy_0" in mesh.shape:
        split = mesh
    else:
        split = Mesh(mesh.devices.reshape(mesh.shape["gx"], 4, 4, 2), AXES)
    dims = tuple(split.shape[a] for a in AXES)
    in_specs = (P(AXES, None, None), P(AXES), P(AXES, None), P(AXES, None), P())
    out_specs = (P(AXES, None), P())
    return jax.shard_map(
        functools.partial(local, dims), mesh=split, in_specs=in_specs, out_specs=out_specs, check_vma=False
    )
```
